16 devices in a mesh: cp: 16 (over z, y, x, core).
Axes of the slice: x: 2, y: 2, z: 2, core: 2. Of those that a mesh axis runs over, the one named last changes fastest.
Arguments:
- hidden_in: bfloat16 [2, 6144, 2048], P(None, 'cp')
- grad_out: bfloat16 [2, 6144, 2048], P(None, 'cp')
- w_query: bfloat16 [2048, 4096], replicated
- w_key: bfloat16 [2048, 512], replicated
- w_value: bfloat16 [2048, 512], replicated
- w_out: bfloat16 [4096, 2048], replicated
- attn_norm: bfloat16 [2048], replicated
- query_norm: bfloat16 [128], replicated
- key_norm: bfloat16 [128], replicated
Outputs:
- output 1: bfloat16 [2, 6144, 2048], P(None, 'cp')
- output 2: bfloat16 [2, 6144, 2048], P(None, 'cp')
- output 3: float32 [2048, 4096], replicated
- output 4: float32 [2048, 512], replicated
- output 5: float32 [2048, 512], replicated
- output 6: float32 [4096, 2048], replicated
- output 7: float32 [2048], replicated
- output 8: float32 [128], replicated
- output 9: float32 [128], replicated
All inputs are finite; a program needn't handle non-finite values.
Results may differ from the reference program's by a relative error of at most 0.017287.
Values are sent between devices in bfloat16 or wider.
A program may use at most 1 GiB of HBM per device.

```python
import jax
import jax.numpy as jnp
from jax import lax

BATCH_SIZE = 2
SEQ_LEN = 6144
MODEL_DIM = 2048
NUM_HEADS = 32
NUM_KV_HEADS = 4
HEAD_DIM = 128
ROW_BLOCK = 128
ROPE_THETA = 1000000.0
NORM_EPS = 1e-6


def setup_inputs(seed: int = 0) -> dict:
    key_list = jax.random.split(jax.random.key(seed), 9)
    q_width = NUM_HEADS * HEAD_DIM
    kv_width = NUM_KV_HEADS * HEAD_DIM
    act_shape = (BATCH_SIZE, SEQ_LEN, MODEL_DIM)
    drawn = {
        'hidden_in': jax.random.normal(key_list[0], act_shape, jnp.float32),
        'grad_out': jax.random.normal(key_list[1], act_shape, jnp.float32),
        'w_query': jax.random.normal(key_list[2], (MODEL_DIM, q_width), jnp.float32) * MODEL_DIM ** -0.5,
        'w_key': jax.random.normal(key_list[3], (MODEL_DIM, kv_width), jnp.float32) * MODEL_DIM ** -0.5,
        'w_value': jax.random.normal(key_list[4], (MODEL_DIM, kv_width), jnp.float32) * MODEL_DIM ** -0.5,
        'w_out': jax.random.normal(key_list[5], (q_width, MODEL_DIM), jnp.float32) * q_width ** -0.5,
        'attn_norm': 1.0 + 0.3 * jax.random.normal(key_list[6], (MODEL_DIM,), jnp.float32),
        'query_norm': 1.75 + 0.3 * jax.random.normal(key_list[7], (HEAD_DIM,), jnp.float32),
        'key_norm': 1.75 + 0.3 * jax.random.normal(key_list[8], (HEAD_DIM,), jnp.float32),
    }
    return {arr_name: arr_val.astype(jnp.bfloat16) for arr_name, arr_val in drawn.items()}


def rms_scale(act_vals, norm_gain):
    mean_sq = jnp.mean(act_vals * act_vals, axis=-1, keepdims=True)
    return act_vals * lax.rsqrt(mean_sq + NORM_EPS) * norm_gain


def rope_tables():
    inv_freq = ROPE_THETA ** (-jnp.arange(0, HEAD_DIM, 2, dtype=jnp.float32) / HEAD_DIM)
    positions = jnp.arange(SEQ_LEN).astype(jnp.float32)
    angles = positions[:, None] * inv_freq[None, :]
    angles = jnp.concatenate([angles, angles], axis=-1)
    return jnp.cos(angles), jnp.sin(angles)


def head_finish(pre_proj, norm_gain, cos_t, sin_t):
    normed = rms_scale(pre_proj, norm_gain)
    half_dim = HEAD_DIM // 2
    rotated = jnp.concatenate([-normed[..., half_dim:], normed[..., :half_dim]], axis=-1)
    return normed * cos_t[:, None, :] + rotated * sin_t[:, None, :]


def block_forward(hidden_in, w_query, w_key, w_value, w_out, attn_norm, query_norm, key_norm):
    group_size = NUM_HEADS // NUM_KV_HEADS
    score_scale = HEAD_DIM ** -0.5
    num_blocks = SEQ_LEN // ROW_BLOCK
    hidden = hidden_in.astype(jnp.float32)
    normed = rms_scale(hidden, attn_norm).astype(jnp.bfloat16).astype(jnp.float32)
    cos_t, sin_t = rope_tables()
    q_pre = jnp.einsum('bsd,df->bsf', normed, w_query).reshape(BATCH_SIZE, SEQ_LEN, NUM_HEADS, HEAD_DIM)
    k_pre = jnp.einsum('bsd,df->bsf', normed, w_key).reshape(BATCH_SIZE, SEQ_LEN, NUM_KV_HEADS, HEAD_DIM)
    v_pre = jnp.einsum('bsd,df->bsf', normed, w_value).reshape(BATCH_SIZE, SEQ_LEN, NUM_KV_HEADS, HEAD_DIM)
    query_rot = head_finish(q_pre, query_norm, cos_t, sin_t).astype(jnp.bfloat16)
    key_rot = head_finish(k_pre, key_norm, cos_t, sin_t).astype(jnp.bfloat16)
    values = v_pre.astype(jnp.bfloat16)
    positions = jnp.arange(SEQ_LEN)
    starts = jnp.arange(num_blocks) * ROW_BLOCK

    def one_sequence(seq_args):
        q_seq, k_seq, v_seq = seq_args
        k_wide = k_seq.astype(jnp.float32)
        v_wide = v_seq.astype(jnp.float32)
        q_blocks = q_seq.reshape(num_blocks, ROW_BLOCK, NUM_KV_HEADS, group_size, HEAD_DIM)

        @jax.checkpoint
        def one_block(blk_args):
            q_blk, row_start = blk_args
            scores = jnp.einsum('qkgd,skd->kgqs', q_blk.astype(jnp.float32), k_wide) * score_scale
            allowed = (row_start + jnp.arange(ROW_BLOCK))[:, None] >= positions[None, :]
            prob_rows = jax.nn.softmax(jnp.where(allowed, scores, -jnp.inf), axis=-1)
            return jnp.einsum('kgqs,skd->qkgd', prob_rows, v_wide)

        block_outs = lax.map(one_block, (q_blocks, starts))
        return block_outs.reshape(SEQ_LEN, NUM_HEADS * HEAD_DIM)

    attn_out = lax.map(one_sequence, (query_rot, key_rot, values)).astype(jnp.bfloat16)
    projected = jnp.einsum('bsf,fd->bsd', attn_out.astype(jnp.float32), w_out)
    return (hidden + projected).astype(jnp.bfloat16)


def reference(hidden_in, grad_out, w_query, w_key, w_value, w_out, attn_norm, query_norm, key_norm):
    hidden_out, pullback = jax.vjp(block_forward, hidden_in, w_query.astype(jnp.float32), w_key.astype(jnp.float32), w_value.astype(jnp.float32), w_out.astype(jnp.float32), attn_norm.astype(jnp.float32), query_norm.astype(jnp.float32), key_norm.astype(jnp.float32))
    grad_list = pullback(grad_out)
    return (hidden_out, grad_list[0], grad_list[1], grad_list[2], grad_list[3], grad_list[4], grad_list[5], grad_list[6], grad_list[7])
```

```python
import functools
import math

import jax
import jax.numpy as jnp
from jax import lax
from jax.experimental import pallas as pl
from jax.experimental.pallas import tpu as pltpu
from jax.sharding import PartitionSpec as P


ROPE_THETA = 1000000.0
NORM_EPS = 1e-6
HEAD_DIM=128; F32=jnp.float32; BF16=jnp.bfloat16
SCALE = HEAD_DIM ** -0.5
EXP2_SCALE = SCALE * math.log2(math.e)
UR = 256


def nn(a, b): return lax.dot_general(a, b, (((1,), (0,)), ((), ())), preferred_element_type=F32)


def nt(a, b): return lax.dot_general(a, b, (((1,), (1,)), ((), ())), preferred_element_type=F32)


def lanes(i): return slice(i * HEAD_DIM, (i + 1) * HEAD_DIM)


def params(**more):
    return pltpu.CompilerParams(dimension_semantics=("arbitrary",), vmem_limit_bytes=60000000, **more)


def cost(flops, nbytes):
    return pl.CostEstimate(flops=flops, bytes_accessed=nbytes, transcendentals=0)


def whole(a):
    return pl.BlockSpec(a.shape, lambda t: (0,) * a.ndim)


def peers_of(kind, me):
    return [me ^ k for k in range(1, 16)] if kind == "all" else [me ^ {"pair": 2, "core": 1}[kind]]


def carrying(kernel, n_in, n_out, n_scratch, steps, kinds):
    if not kinds:
        return kernel
    m = len(kinds)

    def body(*refs):
        ins, srcs, refs = refs[:n_in], refs[n_in:n_in + m], refs[n_in + m:]
        outs, dsts, refs = refs[:n_out], refs[n_out:n_out + m], refs[n_out + m:]
        scratch, sems = refs[:n_scratch], refs[n_scratch:]
        step = pl.program_id(0)
        me = lax.axis_index('cp')

        def copies():
            made = []
            for i, kind in enumerate(kinds):
                send, recv, own = sems[3 * i:3 * i + 3]
                for n, peer in enumerate(peers_of(kind, me)):
                    src, dst = (srcs[i].at[peer], dsts[i].at[me]) if kind == "all" else (srcs[i], dsts[i])
                    made.append(pltpu.make_async_remote_copy(src_ref=src, dst_ref=dst, send_sem=send.at[n], recv_sem=recv.at[n],
                                                             device_id=(peer,), device_id_type=pl.DeviceIdType.MESH))
                if kind == "all":
                    made.append(pltpu.make_async_copy(srcs[i].at[me], dsts[i].at[me], own))
            return made

        @pl.when(step == 0)
        def _():
            barrier = pltpu.get_barrier_semaphore()
            flips = sorted({k for kind in kinds for k in (range(1, 16) if kind == "all" else [{"pair": 2, "core": 1}[kind]])})
            for k in flips:
                pl.semaphore_signal(barrier, inc=1, device_id=(me ^ k,), device_id_type=pl.DeviceIdType.MESH)
            pl.semaphore_wait(barrier, len(flips))
            for copy in copies():
                copy.start()

        kernel(*ins, *outs, *scratch)

        @pl.when(step == steps - 1)
        def _():
            for copy in copies():
                copy.wait()

    return body


def call(kernel, grid, in_specs, out_specs, out_shape, scratch, estimate, operands, carry=(), key=None):
    kinds = [kind for kind, _ in carry]
    hbm = pl.BlockSpec(memory_space=pltpu.HBM)
    sems = []
    for kind in kinds:
        count = 15 if kind == "all" else 1
        sems += [pltpu.SemaphoreType.DMA((count,)), pltpu.SemaphoreType.DMA((count,)), pltpu.SemaphoreType.DMA]
    more = dict(collective_id=key, has_side_effects=True) if kinds else {}
    return pl.pallas_call(
        carrying(kernel, len(operands), len(out_shape), len(scratch), grid, kinds), grid=(grid,),
        in_specs=list(in_specs) + [hbm] * len(kinds), out_specs=list(out_specs) + [hbm] * len(kinds),
        out_shape=list(out_shape) + [jax.ShapeDtypeStruct(a.shape, a.dtype) for _, a in carry],
        scratch_shapes=list(scratch) + sems, compiler_params=params(**more), cost_estimate=estimate,
    )(*operands, *[a for _, a in carry])


def key_mask(width):
    return lax.broadcasted_iota(jnp.int32, (UR, width), 0) + (width - UR) >= lax.broadcasted_iota(jnp.int32, (UR, width), 1)


def flash_fwd_kernel(nh, rh, tk, q_ref, kt_ref, v_ref, o_ref, lse_ref, s_ref, acc_ref, m_ref, l_ref):
    tile = pl.program_id(0)
    tq = rh * UR
    classes = tk // tq
    units = [(r, head) for r in range(rh) for head in range(nh)]
    m_ref[...] = jnp.full_like(m_ref, -jnp.inf)
    l_ref[...] = jnp.zeros_like(l_ref)
    acc_ref[...] = jnp.zeros_like(acc_ref)
    query = lambda u: q_ref[u[0] * UR:(u[0] + 1) * UR, lanes(u[1])]
    for n, u in enumerate(units):
        s_ref[n] = nn(query(u), kt_ref[:, :tk])

    def update(n, keys, scores, width):
        top = scores[:, :HEAD_DIM]
        for piece in range(1, width // HEAD_DIM):
            top = jnp.maximum(top, scores[:, lanes(piece)])
        m_prev = m_ref[n]
        m_new = jnp.maximum(m_prev, jnp.max(top, axis=-1, keepdims=True))
        alpha = jnp.exp2((m_prev - m_new) * EXP2_SCALE)
        shift = m_new * EXP2_SCALE
        part, pieces = None, []
        for piece in range(width // HEAD_DIM):
            prob = jnp.exp2(scores[:, lanes(piece)] * EXP2_SCALE - shift)
            part = prob if part is None else part + prob
            pieces.append(prob.astype(BF16))
        m_ref[n] = m_new
        l_ref[n] = l_ref[n] * alpha + part
        acc_ref[n] = acc_ref[n] * alpha + nn(jnp.concatenate(pieces, axis=1), v_ref[keys, :])

    last = tile // classes

    @pl.loop(0, last)
    def _(j):
        keys = pl.ds(pl.multiple_of(j * tk, tk), tk)
        following = pl.ds(pl.multiple_of(j * tk + tk, tk), tk)
        for n, u in enumerate(units):
            update(n, keys, s_ref[n], tk)
            s_ref[n] = nn(query(u), kt_ref[:, following])

    for c in range(classes):
        @pl.when(tile % classes == c)
        def _():
            for n, u in enumerate(units):
                width = c * tq + (u[0] + 1) * UR
                keys = pl.ds(pl.multiple_of(last * tk, tk), width)
                update(n, keys, jnp.where(key_mask(width), s_ref[n, :, :width], -jnp.inf), width)

    for n, u in enumerate(units):
        rows = slice(u[0] * UR, (u[0] + 1) * UR)
        total = jnp.sum(l_ref[n], axis=-1, keepdims=True)
        o_ref[rows, lanes(u[1])] = (acc_ref[n] / total).astype(BF16)
        lse_ref[rows, lanes(u[1])] = m_ref[n] * EXP2_SCALE + jnp.log2(total)


def run_fwd(q, kt, v, chunk, nh, rh, tk, carry=(), key=None):
    seq, width, tq = q.shape[0], nh * HEAD_DIM, rh * UR
    out = pl.BlockSpec((tq, width), lambda t: (t, 0))
    stat = pltpu.VMEM((nh * rh, UR, HEAD_DIM), F32)
    sds = jax.ShapeDtypeStruct
    return call(functools.partial(flash_fwd_kernel, nh, rh, tk), seq // tq,
                [pl.BlockSpec((tq, width), lambda t: (t, chunk)), whole(kt), whole(v)], [out, out], [sds((seq, width), BF16), sds((seq, width), F32)],
                [pltpu.VMEM((nh * rh, UR, tk), F32), stat, stat, stat], cost(2 * seq * seq * width, seq * 4096), (q, kt, v), carry, key)


def flash_bwd_kernel(nh, rh, tk, q_ref, do_ref, o_ref, lse_ref, kt_ref, vt_ref, k_ref, dq_ref, dkt_ref, dvt_ref, acc_ref, qt_ref, dot_ref, delta_ref, p_ref, ds_ref):
    tile = pl.program_id(0)
    tq = rh * UR
    classes = tk // tq
    units = [(r, head) for r in range(rh) for head in range(nh)]
    rows_of = lambda u: slice(u[0] * UR, (u[0] + 1) * UR)
    at = lambda n: slice(n * UR, (n + 1) * UR)

    @pl.when(tile == 0)
    def _():
        dkt_ref[...] = jnp.zeros_like(dkt_ref)
        dvt_ref[...] = jnp.zeros_like(dvt_ref)

    acc_ref[...] = jnp.zeros_like(acc_ref)
    for n, u in enumerate(units):
        qt_ref[:, at(n)] = q_ref[rows_of(u), lanes(u[1])].astype(F32).T.astype(BF16)
        do = do_ref[rows_of(u), lanes(u[1])].astype(F32)
        dot_ref[:, at(n)] = do.T.astype(BF16)
        delta = jnp.sum(do * o_ref[rows_of(u), lanes(u[1])].astype(F32), axis=-1, keepdims=True)
        delta_ref[n] = jnp.broadcast_to(delta, (UR, HEAD_DIM))

    def unit(n, u, keys, width, masked):
        scores = nn(q_ref[rows_of(u), lanes(u[1])], kt_ref[:, keys])
        if masked:
            scores = jnp.where(key_mask(width), scores, -jnp.inf)
        d_prob = nn(do_ref[rows_of(u), lanes(u[1])], vt_ref[:, keys])
        lse, delta = lse_ref[rows_of(u), lanes(u[1])], delta_ref[n]
        for piece in range(width // HEAD_DIM):
            prob = jnp.exp2(scores[:, lanes(piece)] * EXP2_SCALE - lse)
            p_ref[at(n), lanes(piece)] = prob.astype(BF16)
            ds_ref[at(n), lanes(piece)] = (prob * (d_prob[:, lanes(piece)] - delta)).astype(BF16)

    def products(rows, keys, width):
        dvt_ref[:, keys] += nn(dot_ref[:, rows], p_ref[rows, :width])
        dkt_ref[:, keys] += nn(qt_ref[:, rows], ds_ref[rows, :width])
        acc_ref[rows, :] += nn(ds_ref[rows, :width], k_ref[keys, :])

    last = tile // classes

    @pl.loop(0, last)
    def _(j):
        keys = pl.ds(pl.multiple_of(j * tk, tk), tk)
        for n, u in enumerate(units):
            unit(n, u, keys, tk, False)
        products(slice(0, len(units) * UR), keys, tk)

    for c in range(classes):
        @pl.when(tile % classes == c)
        def _():
            for r in range(rh):
                width = c * tq + (r + 1) * UR
                keys = pl.ds(pl.multiple_of(last * tk, tk), width)
                for n, u in enumerate(units):
                    if u[0] == r:
                        unit(n, u, keys, width, True)
                products(slice(r * nh * UR, (r + 1) * nh * UR), keys, width)

    for n, u in enumerate(units):
        dq_ref[rows_of(u), lanes(u[1])] = (acc_ref[at(n), :] * SCALE).astype(BF16)

    @pl.when(tile == pl.num_programs(0) - 1)
    def _():
        dkt_ref[...] = dkt_ref[...] * SCALE


def run_bwd(q, do, o, lse, kt, vt, k, chunk, nh, rh, tk, carry=(), key=None):
    seq, width, tq, rows = q.shape[0], nh * HEAD_DIM, rh * UR, nh * rh * UR
    row = pl.BlockSpec((tq, width), lambda t: (t, 0))
    sds = jax.ShapeDtypeStruct
    return call(functools.partial(flash_bwd_kernel, nh, rh, tk), seq // tq,
                [pl.BlockSpec((tq, width), lambda t: (t, chunk)), row, row, row, whole(kt), whole(vt), whole(k)], [row, whole(kt), whole(kt)],
                [sds((seq, width), BF16), sds(kt.shape, F32), sds(kt.shape, F32)],
                [pltpu.VMEM((rows, HEAD_DIM), F32), pltpu.VMEM((HEAD_DIM, rows), BF16), pltpu.VMEM((HEAD_DIM, rows), BF16),
                 pltpu.VMEM((nh * rh, UR, HEAD_DIM), F32), pltpu.VMEM((rows, tk), BF16), pltpu.VMEM((rows, tk), BF16)],
                cost(5 * seq * seq * width, seq * 8192), (q, do, o, lse, kt, vt, k), carry, key)


def tn(a, b):
    return nn(a.astype(F32).T.astype(BF16), b)


def rope_tables(offset, length):
    inv_freq = ROPE_THETA ** (-jnp.arange(0, HEAD_DIM, 2, dtype=F32) / HEAD_DIM)
    angles = (offset + jnp.arange(length)).astype(F32)[:, None] * inv_freq[None, :]
    cos_t, sin_t = jnp.cos(angles), jnp.sin(angles)
    return jnp.concatenate([cos_t, cos_t], axis=-1), jnp.concatenate([-sin_t, sin_t], axis=-1)


def half_roll(x):
    return pltpu.roll(x, HEAD_DIM // 2, 1)


def head_finish(pre, gain, cos_t, sin_t):
    scale = lax.rsqrt(jnp.mean(pre * pre, axis=-1, keepdims=True) + NORM_EPS)
    normed = pre * scale * gain
    return normed * cos_t + half_roll(normed) * sin_t


def head_finish_bwd(pre, gain, cos_t, sin_t, d_rot):
    d_normed = d_rot * cos_t - half_roll(d_rot) * sin_t
    scale = lax.rsqrt(jnp.mean(pre * pre, axis=-1, keepdims=True) + NORM_EPS)
    unit = pre * scale
    d_unit = d_normed * gain
    return scale * (d_unit - unit * jnp.mean(d_unit * unit, axis=-1, keepdims=True)), d_normed * unit


def slot_of(tok):
    return ((tok // 4) * 2 + tok % 2) * 2 + (tok // 2) % 2


def qkv_kernel(x_ref, gain_ref, w_ref, qn_ref, kn_ref, cos_ref, sin_ref, h_ref, qpre_ref, kpre_ref, q_ref, k_ref, kt_ref, v_ref, vt_ref):
    rows = x_ref.shape[1]
    step = rows // 3
    for first in range(0, rows, step):
        rs = slice(first, first + step)
        x = x_ref[0, rs].astype(F32)
        scale = lax.rsqrt(jnp.mean(x * x, axis=-1, keepdims=True) + NORM_EPS)
        h = (x * scale * gain_ref[...]).astype(BF16)
        h_ref[rs] = h
        pre = nn(h, w_ref[...])
        cos_t, sin_t = cos_ref[rs], sin_ref[rs]
        qpre_ref[rs] = pre[:, :4 * HEAD_DIM]
        for head in range(4):
            q_ref[rs, lanes(head)] = head_finish(pre[:, lanes(head)], qn_ref[...], cos_t, sin_t).astype(BF16)
        kpre = pre[:, lanes(4)]
        kpre_ref[rs] = kpre
        k_rot = head_finish(kpre, kn_ref[...], cos_t, sin_t)
        k_ref[rs] = k_rot.astype(BF16)
        kt_ref[:, rs] = k_rot.T.astype(BF16)
        v = pre[:, lanes(5)]
        v_ref[rs] = v.astype(BF16)
        vt_ref[:, rs] = v.T.astype(BF16)


def run_qkv(xg, gain, w_all, qn, kn, cos_t, sin_t):
    blocks, rows, dim = xg.shape
    seq = blocks * rows
    row = lambda width: pl.BlockSpec((rows, width), lambda t: (t, 0))
    col = pl.BlockSpec((HEAD_DIM, rows), lambda t: (0, t))
    sds = jax.ShapeDtypeStruct
    return pl.pallas_call(
        qkv_kernel, grid=(blocks,), name="qkv",
        in_specs=[pl.BlockSpec((1, rows, dim), lambda t: (slot_of(t), 0, 0)), whole(gain), whole(w_all), whole(qn), whole(kn), row(HEAD_DIM), row(HEAD_DIM)],
        out_specs=[row(dim), row(4 * HEAD_DIM), row(HEAD_DIM), row(4 * HEAD_DIM), row(HEAD_DIM), col, row(HEAD_DIM), col],
        out_shape=[sds((seq, dim), BF16), sds((seq, 4 * HEAD_DIM), F32), sds((seq, HEAD_DIM), F32), sds((seq, 4 * HEAD_DIM), BF16),
                   sds((seq, HEAD_DIM), BF16), sds((HEAD_DIM, seq), BF16), sds((seq, HEAD_DIM), BF16), sds((HEAD_DIM, seq), BF16)],
        compiler_params=params(), cost_estimate=cost(2 * seq * dim * 768, seq * dim * 8),
    )(xg, gain, w_all, qn, kn, cos_t, sin_t)


def out_grad_kernel(g_ref, w_ref, o_ref, do_ref, wg_ref):
    g = g_ref[0]
    do_ref[...] = nn(g, w_ref[...]).astype(BF16)

    @pl.when(pl.program_id(0) == 0)
    def _():
        wg_ref[...] = jnp.zeros_like(wg_ref)

    wg_ref[...] += tn(o_ref[...], g)


def run_out_grad(gg, wo, o):
    blocks, rows, dim = gg.shape
    width = wo.shape[1]
    row = pl.BlockSpec((rows, width), lambda t: (t, 0))
    return pl.pallas_call(
        out_grad_kernel, grid=(blocks,), name="out_grad",
        in_specs=[pl.BlockSpec((1, rows, dim), lambda t: (slot_of(t), 0, 0)), whole(wo), row], out_specs=[row, pl.BlockSpec((width, dim), lambda t: (0, 0))],
        out_shape=[jax.ShapeDtypeStruct(o.shape, BF16), jax.ShapeDtypeStruct((width, dim), F32)],
        compiler_params=params(), cost_estimate=cost(4 * blocks * rows * dim * width, blocks * rows * dim * 2),
    )(gg, wo, o)


def in_grad_kernel(with_kv, *refs):
    if with_kv:
        dq_ref, qpre_ref, qn_ref, cos_ref, sin_ref, h_ref, kv_ref, kpre_ref, kn_ref, half_ref, wg_ref, kvb_ref, dt_ref = refs
    else:
        dq_ref, qpre_ref, qn_ref, cos_ref, sin_ref, h_ref, wg_ref, dt_ref = refs

    @pl.when(pl.program_id(0) == 0)
    def _():
        wg_ref[...] = jnp.zeros_like(wg_ref)
        dt_ref[...] = jnp.zeros_like(dt_ref)

    wg_ref[...] += nn(dt_ref[...], h_ref[...])
    cos_t, sin_t = cos_ref[...], sin_ref[...]
    for head in range(2):
        d_pre, _ = head_finish_bwd(qpre_ref[:, lanes(head)], qn_ref[...], cos_t, sin_t, dq_ref[:, lanes(head)].astype(F32))
        dt_ref[lanes(head), :] = d_pre.T.astype(BF16)
    if with_kv:
        kv = kv_ref[...].T.astype(BF16)
        kvb_ref[...] = kv
        dk_pre, _ = head_finish_bwd(kpre_ref[...], kn_ref[...], cos_t, sin_t, kv.astype(F32))
        dt_ref[lanes(2), :] = jnp.where(half_ref[0] == 0, dk_pre, kv.astype(F32)).T.astype(BF16)


def run_in_grad(dq, qpre, chunk, qn, cos_t, sin_t, h, kv=None, carry=(), key=None):
    seq, dim = h.shape
    rows = 512
    count = seq // rows
    row = lambda width, c=0: pl.BlockSpec((rows, width), lambda t: (jnp.minimum(t, count - 1), c))
    operands = [dq, qpre, qn, cos_t, sin_t, h]
    specs = [row(256), row(256, chunk), whole(qn), row(HEAD_DIM), row(HEAD_DIM), pl.BlockSpec((rows, dim), lambda t: (jnp.maximum(t - 1, 0), 0))]
    height = 256
    out_specs, out_shape = [], []
    if kv is not None:
        kv_sum, kpre, kn, half = kv
        operands += [kv_sum, kpre, kn, half]
        specs += [pl.BlockSpec((HEAD_DIM, rows), lambda t: (0, jnp.minimum(t, count - 1))), row(HEAD_DIM), whole(kn), pl.BlockSpec(memory_space=pltpu.SMEM)]
        height = 384
        out_specs, out_shape = [row(HEAD_DIM)], [jax.ShapeDtypeStruct((seq, HEAD_DIM), BF16)]
    return call(functools.partial(in_grad_kernel, kv is not None), count + 1, specs, [pl.BlockSpec((height, dim), lambda t: (0, 0))] + out_specs,
                [jax.ShapeDtypeStruct((height, dim), F32)] + out_shape, [pltpu.VMEM((height, rows), BF16)], cost(2 * seq * dim * height, seq * dim * 3), operands, carry, key)


def out_proj_kernel(o0_ref, o1_ref, wa_ref, wb_ref, x_ref, y_ref, acc_ref):
    step = pl.program_id(0)

    @pl.when(step == 0)
    def _():
        acc_ref[...] = jnp.zeros_like(acc_ref)

    rows = x_ref.shape[1]
    o0, o1 = o0_ref[0, :, 0].reshape(2 * rows, 256), o1_ref[0, :, 0].reshape(2 * rows, 256)
    for j, w_ref in ((0, wa_ref), (1, wb_ref)):
        pair = jnp.concatenate([o0[:, lanes(j)], o1[:, lanes(j)]], axis=1)
        acc_ref[...] += nn(pair, w_ref[...])

    @pl.when(step == pl.num_programs(0) - 1)
    def _():
        for b in range(2):
            y_ref[b] = (x_ref[b].astype(F32) + acc_ref[b * rows:(b + 1) * rows, :]).astype(BF16)


def run_out_proj(o_got, w_out, hidden_in, carry=(), key=None):
    batch, rows, dim = hidden_in.shape
    src = pl.BlockSpec((1, 2, 1, rows, 256), lambda s: (s // 2, 0, s % 2, 0, 0))
    w_spec = lambda j: pl.BlockSpec((256, dim), lambda s: (4 * (s // 2) + 2 * j + s % 2, 0))
    return call(out_proj_kernel, 8, [src, src, w_spec(0), w_spec(1), whole(hidden_in)], [whole(hidden_in)],
                [jax.ShapeDtypeStruct(hidden_in.shape, BF16)], [pltpu.VMEM((batch * rows, dim), F32)],
                cost(2 * batch * rows * dim * 4096, 30000000), (o_got[0], o_got[1], w_out, w_out, hidden_in), carry, key)


def hidden_grad_kernel(dq0_ref, dq1_ref, kv_ref, qa_ref, qb_ref, kpre_ref, wqa_ref, wqb_ref, wk_ref, wv_ref, qn_ref, kn_ref, gain_ref,
                       cos_ref, sin_ref, x_ref, g_ref, dx_ref, ngq_ref, ngk_ref, ngx_ref, acc_ref):
    step = pl.program_id(0)
    rows = x_ref.shape[1]

    @pl.when(step == 0)
    def _():
        acc_ref[...] = jnp.zeros_like(acc_ref)
        ngq_ref[...] = jnp.zeros_like(ngq_ref)
        ngk_ref[...] = jnp.zeros_like(ngk_ref)

    is_key = step % 2 == 0
    cos_t = jnp.concatenate([cos_ref[...]] * 2, axis=0)
    sin_t = jnp.concatenate([sin_ref[...]] * 2, axis=0)
    dq0, dq1 = dq0_ref[0, :, 0].reshape(2 * rows, 256), dq1_ref[0, :, 0].reshape(2 * rows, 256)
    total = None
    for j, (q_ref, w_ref) in enumerate(((qa_ref, wqa_ref), (qb_ref, wqb_ref))):
        parts = []
        for c, dq in ((0, dq0), (1, dq1)):
            d_pre, terms = head_finish_bwd(q_ref[:, lanes(c)], qn_ref[...], cos_t, sin_t, dq[:, lanes(j)].astype(F32))
            parts.append(d_pre.astype(BF16))
            ngq_ref[...] += jnp.sum(terms.reshape(-1, 8, HEAD_DIM), axis=0)
        part = nt(jnp.concatenate(parts, axis=1), w_ref[...])
        total = part if total is None else total + part
    kv = kv_ref[0, :, 0].reshape(2 * rows, HEAD_DIM).astype(F32)
    dk_pre, terms = head_finish_bwd(kpre_ref[...], kn_ref[...], cos_t, sin_t, kv)
    ngk_ref[...] += jnp.where(is_key, jnp.sum(terms.reshape(-1, 8, HEAD_DIM), axis=0), 0.0)
    w_kv = jnp.where(is_key, wk_ref[...].astype(F32), wv_ref[...].astype(F32)).astype(BF16)
    acc_ref[...] += total + nt(jnp.where(is_key, dk_pre, kv).astype(BF16), w_kv)

    @pl.when(step == pl.num_programs(0) - 1)
    def _():
        partial = None
        for b in range(2):
            for r in range(0, rows, 64):
                rs = slice(r, r + 64)
                x = x_ref[b, rs].astype(F32)
                scale = lax.rsqrt(jnp.mean(x * x, axis=-1, keepdims=True) + NORM_EPS)
                unit = x * scale
                d_normed = acc_ref[b * rows + r:b * rows + r + 64, :].astype(BF16).astype(F32)
                terms = jnp.sum((d_normed * unit).reshape(8, 8, x.shape[1]), axis=0)
                partial = terms if partial is None else partial + terms
                d_unit = d_normed * gain_ref[...]
                d_x = scale * (d_unit - unit * jnp.mean(d_unit * unit, axis=-1, keepdims=True))
                dx_ref[b, rs] = (g_ref[b, rs].astype(F32) + d_x).astype(BF16)
        ngx_ref[...] = partial


def run_hidden_grad(dq_got, kv_got, qpre_own, kpre_own, w_query, w_key, w_value, qn, kn, gain, cos_t, sin_t, hidden_in, grad_out):
    batch, rows, dim = hidden_in.shape
    src = lambda width: pl.BlockSpec((1, 2, 1, rows, width), lambda s: (s // 2, 0, s % 2, 0, 0))
    cols = lambda height, j: pl.BlockSpec((height, 256), lambda s: (0, 4 * (s // 2) + 2 * j + s % 2))
    group = lambda height: pl.BlockSpec((height, HEAD_DIM), lambda s: (0, s // 2))
    fixed = lambda *shape: pl.BlockSpec(shape, lambda s: (0,) * len(shape))
    sds = jax.ShapeDtypeStruct
    both = batch * rows
    return pl.pallas_call(
        hidden_grad_kernel, grid=(8,), name="hidden_grad",
        in_specs=[src(256), src(256), src(HEAD_DIM), cols(both, 0), cols(both, 1), group(both), cols(dim, 0), cols(dim, 1), group(dim), group(dim),
                  whole(qn), whole(kn), whole(gain), whole(cos_t), whole(sin_t), whole(hidden_in), whole(grad_out)],
        out_specs=[whole(hidden_in), fixed(8, HEAD_DIM), fixed(8, HEAD_DIM), fixed(8, dim)],
        out_shape=[sds(hidden_in.shape, BF16), sds((8, HEAD_DIM), F32), sds((8, HEAD_DIM), F32), sds((8, dim), F32)],
        scratch_shapes=[pltpu.VMEM((both, dim), F32)],
        compiler_params=params(), cost_estimate=cost(2 * both * dim * 5120, 50000000),
    )(dq_got[0], dq_got[1], kv_got, qpre_own, qpre_own, kpre_own, w_query, w_query, w_key, w_value, qn, kn, gain, cos_t, sin_t, hidden_in, grad_out)


def place_kernel(*refs):
    refs[-1][...] = refs[0][0].T


def run_place(a, chunk, into=None):
    count, height, dim = a.shape[0], HEAD_DIM, a.shape[2]
    more = [] if into is None else [into]
    return pl.pallas_call(
        place_kernel, grid=(count,), name="place",
        in_specs=[pl.BlockSpec((1, height, dim), lambda t: (t, 0, 0))] + [pl.BlockSpec(memory_space=pltpu.HBM)] * len(more),
        out_specs=pl.BlockSpec((dim, height), lambda t: (0, 2 * t + chunk)), input_output_aliases={} if into is None else {1: 0},
        out_shape=jax.ShapeDtypeStruct((dim, 2 * height * count), F32), compiler_params=params(), cost_estimate=cost(1000000, 35000000),
    )(a, *more)


def solution(mesh):
    n_dev = mesh.shape['cp']
    seq_spec, rep_spec = P(None, 'cp', None), P()
    flip = lambda bit: [(dev, dev ^ bit) for dev in range(n_dev)]
    halves = [[dev for dev in range(n_dev) if (dev >> 1) & 1 == bit] for bit in (0, 1)]

    def local_block(hidden_in, grad_out, w_query, w_key, w_value, w_out, attn_norm, query_norm, key_norm):
        batch, seq_dev, dim = hidden_in.shape
        seq = seq_dev * n_dev
        kv_heads = w_key.shape[1] // HEAD_DIM
        me = lax.axis_index('cp')
        group, which, half = me // 4, (me // 2) % 2, me % 2
        gain = attn_norm.astype(F32).reshape(1, dim)
        qn, kn = query_norm.astype(F32).reshape(1, HEAD_DIM), key_norm.astype(F32).reshape(1, HEAD_DIM)

        gather_all = lambda x: lax.all_gather(x, 'cp')

        def gather_sequence(local):
            other = lax.dynamic_index_in_dim(local, 1 - which, 0, keepdims=False)
            got = lax.ppermute(other, 'cp', flip(2))
            pair = lax.dynamic_update_index_in_dim(local, got, 1 - which, 0)
            return lax.all_gather(pair, 'cp', axis_index_groups=halves, tiled=True)

        def split(parts):
            keep = lax.dynamic_index_in_dim(parts, which, 0, keepdims=False)
            return keep, lax.dynamic_index_in_dim(parts, 1 - which, 0, keepdims=False)

        blocks = lambda x: x.reshape(n_dev, seq_dev, x.shape[1])
        by_source = lambda x: x.reshape(4, 2, 2, seq_dev, x.shape[2])

        xg = gather_sequence(hidden_in)
        gg = gather_sequence(grad_out)
        cos_t, sin_t = rope_tables(0, seq)

        hidden = hidden_in.astype(F32)
        x_scale = lax.rsqrt(jnp.mean(hidden * hidden, axis=-1, keepdims=True) + NORM_EPS)
        h_own = (hidden * x_scale * gain).astype(BF16).reshape(batch * seq_dev, dim)
        qpre_own = nn(h_own, w_query)
        kpre_own = nn(h_own, w_key)

        head_at = lambda c, j: (8 * group + 4 * j + 2 * half + c) * HEAD_DIM
        order = [(c, j) for c in range(2) for j in range(2)]
        wq_mine = [lax.dynamic_slice_in_dim(w_query, head_at(c, j), HEAD_DIM, 1) for c, j in order]
        wk_mine = lax.dynamic_slice_in_dim(w_key, group * HEAD_DIM, HEAD_DIM, 1)
        wv_mine = lax.dynamic_slice_in_dim(w_value, group * HEAD_DIM, HEAD_DIM, 1)
        w_all = jnp.concatenate(wq_mine + [wk_mine, wv_mine], axis=1)
        wo_mine = [jnp.concatenate([lax.dynamic_slice_in_dim(w_out, head_at(c, j), HEAD_DIM, 0) for j in range(2)], axis=0).T for c in range(2)]

        xg, qpre_own, kpre_own = lax.optimization_barrier((xg, qpre_own, kpre_own))
        h, qpre, kpre, q, k, kt, v, vt = run_qkv(xg, gain, w_all, qn, kn, cos_t, sin_t)

        o0, lse0 = run_fwd(q, kt, v, 0, 2, 2, 1024)
        do0, wg_c = run_out_grad(gg, wo_mine[0], o0)
        keep, give = split(wg_c.reshape(2, HEAD_DIM, dim))
        o1, lse1, o_got0, got = run_fwd(q, kt, v, 1, 2, 2, 1024, [("all", blocks(o0)), ("pair", give)], 1)
        mine, o1 = lax.optimization_barrier((keep + got, o1))
        wg_out0 = gather_all(mine)
        do1, wg_c = run_out_grad(gg, wo_mine[1], o1)
        keep, give = split(wg_c.reshape(2, HEAD_DIM, dim))
        dq0, dkt0, dvt0, o_got1, got = run_bwd(q, do0, o0, lse0, kt, vt, k, 0, 2, 2, 1024, [("all", blocks(o1)), ("pair", give)], 2)
        mine, dq0 = lax.optimization_barrier((keep + got, dq0))
        wg_out1 = gather_all(mine)
        wgrad_out = jnp.stack([wg_out0, wg_out1], axis=1).reshape(w_out.shape)

        wg_c, = run_in_grad(dq0, qpre, 0, qn, cos_t, sin_t, h)
        keep, give = split(wg_c.reshape(2, HEAD_DIM, dim))
        dq1, dkt1, dvt1, dq_got0, got = run_bwd(q, do1, o1, lse1, kt, vt, k, 1, 2, 2, 1024, [("all", blocks(dq0)), ("pair", give)], 3)
        mine, dq1 = lax.optimization_barrier((keep + got, dq1))
        wg_q0 = gather_all(mine)
        dkt, dvt = dkt0 + dkt1, dvt0 + dvt1
        kv_keep, kv_give = jnp.where(half == 0, dkt, dvt), jnp.where(half == 0, dvt, dkt)
        kv_sum = kv_keep + lax.ppermute(kv_give, 'cp', flip(1))
        half_arr = half.astype(jnp.int32).reshape(1)
        wg_c, kv_b, dq_got1 = run_in_grad(dq1, qpre, 1, qn, cos_t, sin_t, h, (kv_sum, kpre, kn, half_arr), [("all", blocks(dq1))], 4)
        keep, give = split(jnp.concatenate([wg_c[:256].reshape(2, HEAD_DIM, dim), wg_c[256:].reshape(2, HEAD_DIM // 2, dim)], axis=1))
        hidden_out, kv_got, got = run_out_proj([by_source(o_got0), by_source(o_got1)], w_out, hidden_in, [("all", blocks(kv_b)), ("pair", give)], 5)
        mine, qpre_own = lax.optimization_barrier((keep + got, qpre_own))
        wg_q1 = gather_all(mine)
        wgrad_q = run_place(wg_q1, 1, run_place(wg_q0, 0))
        wg_kv = wg_q1[:, HEAD_DIM:].reshape(4, 2, 2, HEAD_DIM // 2, dim).transpose(2, 4, 0, 1, 3).reshape(2, dim, kv_heads * HEAD_DIM)
        dq_got, kv_got = [by_source(dq_got0), by_source(dq_got1)], by_source(kv_got)

        my_cos, my_sin = rope_tables(me * seq_dev, seq_dev)
        grad_in, ng_q, ng_k, ng_x = run_hidden_grad(dq_got, kv_got, qpre_own, kpre_own, w_query, w_key, w_value, qn, kn, gain, my_cos, my_sin, hidden_in, grad_out)
        norms = jnp.concatenate([jnp.sum(ng_x, axis=0), jnp.sum(ng_q, axis=0), jnp.sum(ng_k, axis=0)])
        norms = lax.psum(norms, 'cp')
        return (hidden_out, grad_in, wgrad_q, wg_kv[0], wg_kv[1], wgrad_out,
                norms[:dim], norms[dim:dim + HEAD_DIM], norms[dim + HEAD_DIM:])

    return jax.shard_map(local_block, mesh=mesh, in_specs=(seq_spec, seq_spec) + (rep_spec,) * 7, out_specs=(seq_spec, seq_spec) + (rep_spec,) * 7, check_vma=False)
```

```python
import functools
import math

import jax
import jax.numpy as jnp
from jax import lax
from jax.experimental import pallas as pl
from jax.experimental.pallas import tpu as pltpu
from jax.sharding import PartitionSpec as P


ROPE_THETA = 1000000.0
NORM_EPS = 1e-6
HEAD_DIM=128; F32=jnp.float32; BF16=jnp.bfloat16
SCALE = HEAD_DIM ** -0.5
EXP2_SCALE = SCALE * math.log2(math.e)
UR = 256
TILING = (2, 2, 1024)


def nn(a, b): return lax.dot_general(a, b, (((1,), (0,)), ((), ())), preferred_element_type=F32)


def nt(a, b): return lax.dot_general(a, b, (((1,), (1,)), ((), ())), preferred_element_type=F32)


def lanes(i): return slice(i * HEAD_DIM, (i + 1) * HEAD_DIM)


def params(**more):
    return pltpu.CompilerParams(dimension_semantics=("arbitrary",), vmem_limit_bytes=60000000, **more)


def cost(flops, nbytes):
    return pl.CostEstimate(flops=flops, bytes_accessed=nbytes, transcendentals=0)


def fixed(*shape):
    return pl.BlockSpec(shape, lambda t: (0,) * len(shape))


def whole(a):
    return fixed(*a.shape)


def row_spec(rows, width, shift=0, col=0):
    return pl.BlockSpec((rows, width), lambda t: (t + shift, col))


def grid_step():
    return pl.program_id(0)


def row_of(reduce, x):
    return reduce(x, axis=-1, keepdims=True)


def row_mean(x):
    return row_of(jnp.mean, x)


def row_scale(x):
    return lax.rsqrt(row_mean(x * x) + NORM_EPS)


SPLIT = 12
OTHERS = tuple(range(1, 16))
FLIPS = {"all": OTHERS, "low": OTHERS, "high": OTHERS, "half": (2,), "other": (1,)}


def carrying(kernel, n_in, n_out, n_scratch, steps, kinds):
    if not kinds:
        return kernel
    m = sum(2 if kind == "other" else 1 for kind in kinds)

    def body(*refs):
        ins, srcs, refs = refs[:n_in], refs[n_in:n_in + m], refs[n_in + m:]
        outs, dsts, refs = refs[:n_out], refs[n_out:n_out + len(kinds)], refs[n_out + len(kinds):]
        scratch, sems = refs[:n_scratch], refs[n_scratch:]
        step = grid_step()
        me = lax.axis_index('cp')

        def remote(src, dst, send, recv, peer):
            return pltpu.make_async_remote_copy(src_ref=src, dst_ref=dst, send_sem=send, recv_sem=recv, device_id=(peer,), device_id_type=pl.DeviceIdType.MESH)

        def each(send_part, recv_part, local_part):
            def act(copy):
                send_part(copy)
                recv_part(copy)

            first = 0
            for i, kind in enumerate(kinds):
                send, recv, own = sems[3 * i:3 * i + 3]
                src, dst = srcs[first], dsts[i]
                if kind == "all":
                    for n, flip in enumerate(FLIPS[kind]):
                        act(remote(src.at[me ^ flip], dst.at[me], send.at[n], recv.at[n], me ^ flip))
                    local_part(pltpu.make_async_copy(src.at[me], dst.at[me], own))
                elif kind in ("low", "high"):
                    base = 0 if kind == "low" else SPLIT
                    chosen = (lambda dev: dev < SPLIT) if kind == "low" else (lambda dev: dev >= SPLIT)
                    for n, flip in enumerate(FLIPS[kind]):
                        peer = me ^ flip

                        @pl.when(chosen(peer))
                        def _():
                            send_part(remote(src.at[peer - base], dst.at[me], send.at[n], recv.at[n], peer))

                        @pl.when(chosen(me))
                        def _():
                            recv_part(remote(src.at[0], dst.at[peer], send.at[n], recv.at[n], peer))

                    @pl.when(chosen(me))
                    def _():
                        local_part(pltpu.make_async_copy(src.at[me - base], dst.at[me], own))
                elif kind == "half":
                    rows = dst.shape[0]
                    theirs = pl.multiple_of((1 - (me // 2) % 2) * rows, rows)
                    act(remote(src.at[pl.ds(theirs, rows)], dst, send.at[0], recv.at[0], me ^ 2))
                else:
                    @pl.when(me % 2 == 0)
                    def _():
                        act(remote(srcs[first + 1], dst, send.at[0], recv.at[0], me ^ 1))

                    @pl.when(me % 2 == 1)
                    def _():
                        act(remote(src, dst, send.at[0], recv.at[0], me ^ 1))

                    first += 1
                first += 1

        @pl.when(step == 0)
        def _():
            meet(me, sorted({flip for kind in kinds for flip in FLIPS[kind]}))
            each(lambda copy: copy.start(), lambda copy: None, lambda copy: copy.start())

        kernel(*ins, *outs, *scratch)

        @pl.when(step == steps - 1)
        def _():
            each(lambda copy: copy.wait_send(), lambda copy: copy.wait_recv(), lambda copy: copy.wait())

    return body


def meet(me, flips):
    barrier = pltpu.get_barrier_semaphore()
    for flip in flips:
        pl.semaphore_signal(barrier, inc=1, device_id=(me ^ flip,), device_id_type=pl.DeviceIdType.MESH)
    pl.semaphore_wait(barrier, len(flips))


def call(kernel, grid, in_specs, out_specs, out_shape, scratch, estimate, operands, carry=(), key=None, aliases=None):
    kinds = [kind for kind, *_ in carry]
    sources = [a for _, *arrays in carry for a in arrays]
    hbm = pl.BlockSpec(memory_space=pltpu.HBM)
    sems, received = [], []
    for kind, a, *_ in carry:
        count = len(FLIPS[kind])
        sems += [pltpu.SemaphoreType.DMA((count,)), pltpu.SemaphoreType.DMA((count,)), pltpu.SemaphoreType.DMA]
        count = a.shape[0] // 2 if kind == "half" else 16 if kind in ("low", "high") else a.shape[0]
        received.append(jax.ShapeDtypeStruct((count,) + a.shape[1:], a.dtype))
    more = dict(collective_id=key, has_side_effects=True) if kinds else {}
    return pl.pallas_call(
        carrying(kernel, len(operands), len(out_shape), len(scratch), grid, kinds), grid=(grid,),
        in_specs=list(in_specs) + [hbm] * len(sources), out_specs=list(out_specs) + [hbm] * len(kinds),
        out_shape=list(out_shape) + received, scratch_shapes=list(scratch) + sems, compiler_params=params(**more), cost_estimate=estimate,
        input_output_aliases=aliases or {},
    )(*operands, *sources)


def key_mask(width):
    return lax.broadcasted_iota(jnp.int32, (UR, width), 0) + (width - UR) >= lax.broadcasted_iota(jnp.int32, (UR, width), 1)


def flash_fwd_kernel(nh, rh, tk, begin, q_ref, kt_ref, v_ref, *refs):
    o_ref, lse_ref, s_ref, acc_ref, m_ref, l_ref = refs[-6:]
    tile = grid_step() + begin
    tq = rh * UR
    classes = tk // tq
    units = [(r, head) for r in range(rh) for head in range(nh)]
    m_ref[:] = jnp.full_like(m_ref, -jnp.inf)
    l_ref[:] = jnp.zeros_like(l_ref)
    acc_ref[:] = jnp.zeros_like(acc_ref)
    query = lambda u: q_ref[u[0] * UR:(u[0] + 1) * UR, lanes(u[1])]
    for n, u in enumerate(units):
        s_ref[n] = nn(query(u), kt_ref[:, :tk])

    def update(n, keys, scores, width):
        top = scores[:, :HEAD_DIM]
        for piece in range(1, width // HEAD_DIM):
            top = jnp.maximum(top, scores[:, lanes(piece)])
        m_prev = m_ref[n]
        m_new = jnp.maximum(m_prev, row_of(jnp.max, top))
        alpha = jnp.exp2((m_prev - m_new) * EXP2_SCALE)
        shift = m_new * EXP2_SCALE
        part, pieces = None, []
        for piece in range(width // HEAD_DIM):
            prob = jnp.exp2(scores[:, lanes(piece)] * EXP2_SCALE - shift)
            part = prob if part is None else part + prob
            pieces.append(prob.astype(BF16))
        m_ref[n] = m_new
        l_ref[n] = l_ref[n] * alpha + part
        acc_ref[n] = acc_ref[n] * alpha + nn(jnp.hstack(pieces), v_ref[keys, :])

    last = tile // classes

    @pl.loop(0, last)
    def _(j):
        keys = pl.ds(pl.multiple_of(j * tk, tk), tk)
        following = pl.ds(pl.multiple_of(j * tk + tk, tk), tk)
        for n, u in enumerate(units):
            update(n, keys, s_ref[n], tk)
            s_ref[n] = nn(query(u), kt_ref[:, following])

    for c in range(classes):
        @pl.when(tile % classes == c)
        def _():
            for n, u in enumerate(units):
                width = c * tq + (u[0] + 1) * UR
                keys = pl.ds(pl.multiple_of(last * tk, tk), width)
                update(n, keys, jnp.where(key_mask(width), s_ref[n, :, :width], -jnp.inf), width)

    for n, u in enumerate(units):
        rows = slice(u[0] * UR, (u[0] + 1) * UR)
        total = row_of(jnp.sum, l_ref[n])
        o_ref[rows, lanes(u[1])] = (acc_ref[n] / total).astype(BF16)
        lse_ref[rows, lanes(u[1])] = m_ref[n] * EXP2_SCALE + jnp.log2(total)


def run_fwd(q, kt, v, chunk, carry=(), key=None, tiles=None, into=()):
    nh, rh, tk = TILING
    seq, width, tq = q.shape[0], nh * HEAD_DIM, rh * UR
    begin, end = tiles or (0, seq // tq)
    out = row_spec(tq, width, begin)
    stat = pltpu.VMEM((nh * rh, UR, HEAD_DIM), F32)
    sds = jax.ShapeDtypeStruct
    share = (end * end - begin * begin) * tq * tq / (seq * seq)
    return call(functools.partial(flash_fwd_kernel, nh, rh, tk, begin), end - begin,
                [row_spec(tq, width, begin, chunk), whole(kt), whole(v)] + [pl.BlockSpec(memory_space=pltpu.HBM)] * len(into), [out, out],
                [sds((seq, width), BF16), sds((seq, width), F32)], [pltpu.VMEM((nh * rh, UR, tk), F32), stat, stat, stat],
                cost(int(2 * seq * seq * width * share), seq * 4096), (q, kt, v, *into), carry, key, {3: 0, 4: 1} if into else None)


def flash_bwd_kernel(nh, rh, tk, begin, end, first, q_ref, do_ref, o_ref, lse_ref, kt_ref, vt_ref, k_ref, *refs):
    dk0_ref, dv0_ref = (None, None) if first else refs[:2]
    dq_ref, dkt_ref, dvt_ref, acc_ref, qt_ref, dot_ref, delta_ref, p_ref, ds_ref = refs[-9:]
    tile = grid_step() + begin
    tq = rh * UR
    classes = tk // tq
    units = [(r, head) for r in range(rh) for head in range(nh)]
    rows_of = lambda u: slice(u[0] * UR, (u[0] + 1) * UR)
    at = lambda n: slice(n * UR, (n + 1) * UR)

    @pl.when(tile == begin)
    def _():
        dkt_ref[:] = jnp.zeros_like(dkt_ref) if first else dk0_ref[:]
        dvt_ref[:] = jnp.zeros_like(dvt_ref) if first else dv0_ref[:]

    acc_ref[:] = jnp.zeros_like(acc_ref)
    for n, u in enumerate(units):
        qt_ref[:, at(n)] = q_ref[rows_of(u), lanes(u[1])].astype(F32).T.astype(BF16)
        do = do_ref[rows_of(u), lanes(u[1])].astype(F32)
        dot_ref[:, at(n)] = do.T.astype(BF16)
        delta = row_of(jnp.sum, do * o_ref[rows_of(u), lanes(u[1])].astype(F32))
        delta_ref[n] = jnp.broadcast_to(delta, (UR, HEAD_DIM))

    def unit(n, u, keys, width, masked):
        scores = nn(q_ref[rows_of(u), lanes(u[1])], kt_ref[:, keys])
        if masked:
            scores = jnp.where(key_mask(width), scores, -jnp.inf)
        d_prob = nn(do_ref[rows_of(u), lanes(u[1])], vt_ref[:, keys])
        lse, delta = lse_ref[rows_of(u), lanes(u[1])], delta_ref[n]
        for piece in range(width // HEAD_DIM):
            prob = jnp.exp2(scores[:, lanes(piece)] * EXP2_SCALE - lse)
            p_ref[at(n), lanes(piece)] = prob.astype(BF16)
            ds_ref[at(n), lanes(piece)] = (prob * (d_prob[:, lanes(piece)] - delta)).astype(BF16)

    def products(rows, keys, width):
        dvt_ref[:, keys] += nn(dot_ref[:, rows], p_ref[rows, :width])
        dkt_ref[:, keys] += nn(qt_ref[:, rows], ds_ref[rows, :width])
        acc_ref[rows, :] += nn(ds_ref[rows, :width], k_ref[keys, :])

    last = tile // classes

    @pl.loop(0, last)
    def _(j):
        keys = pl.ds(pl.multiple_of(j * tk, tk), tk)
        for n, u in enumerate(units):
            unit(n, u, keys, tk, False)
        products(slice(0, len(units) * UR), keys, tk)

    for c in range(classes):
        @pl.when(tile % classes == c)
        def _():
            for r in range(rh):
                width = c * tq + (r + 1) * UR
                keys = pl.ds(pl.multiple_of(last * tk, tk), width)
                for n, u in enumerate(units):
                    if u[0] == r:
                        unit(n, u, keys, width, True)
                products(slice(r * nh * UR, (r + 1) * nh * UR), keys, width)

    for n, u in enumerate(units):
        dq_ref[rows_of(u), lanes(u[1])] = (acc_ref[at(n), :] * SCALE).astype(BF16)

    if end < 0:
        @pl.when(tile == begin + pl.num_programs(0) - 1)
        def _():
            dkt_ref[:] = dkt_ref[:] * SCALE


def run_bwd(q, do, o, lse, kt, vt, k, chunk, carry=(), key=None, so_far=(), tiles=None, last=False, into=None):
    nh, rh, tk = TILING
    seq, width, tq, rows = q.shape[0], nh * HEAD_DIM, rh * UR, nh * rh * UR
    begin, end = tiles or (0, seq // tq)
    row = row_spec(tq, width, begin)
    sds = jax.ShapeDtypeStruct
    share = (end * end - begin * begin) * tq * tq / (seq * seq)
    held, start, height = [], 0, (end - begin) * tq
    if into is not None:
        held, start, height = [] if isinstance(into, str) else [into], begin, seq
    return call(functools.partial(flash_bwd_kernel, nh, rh, tk, begin, -1 if last else 0, not so_far), end - begin,
                [row_spec(tq, width, begin, chunk), row, row, row, whole(kt), whole(vt), whole(k)] + [whole(a) for a in so_far] + [pl.BlockSpec(memory_space=pltpu.HBM)] * len(held),
                [row_spec(tq, width, start), whole(kt), whole(kt)], [sds((height, width), BF16), sds(kt.shape, F32), sds(kt.shape, F32)],
                [pltpu.VMEM((rows, HEAD_DIM), F32), pltpu.VMEM((HEAD_DIM, rows), BF16), pltpu.VMEM((HEAD_DIM, rows), BF16),
                 pltpu.VMEM((nh * rh, UR, HEAD_DIM), F32), pltpu.VMEM((rows, tk), BF16), pltpu.VMEM((rows, tk), BF16)],
                cost(int(5 * seq * seq * width * share), seq * 8192), (q, do, o, lse, kt, vt, k, *so_far, *held), carry, key, {7 + len(so_far): 0} if held else None)


def tn(a, b):
    return nn(a.astype(F32).T.astype(BF16), b)


def inverse_frequencies():
    inv_freq = ROPE_THETA ** (-jnp.arange(0, HEAD_DIM, 2, dtype=F32) / HEAD_DIM)
    return jnp.concatenate([inv_freq, inv_freq]).reshape(1, HEAD_DIM)


def half_roll(x):
    return pltpu.roll(x, HEAD_DIM // 2, 1)


def head_finish(pre, gain, cos_t, sin_t):
    scale = row_scale(pre)
    normed = pre * scale * gain
    return normed * cos_t + half_roll(normed) * sin_t


def head_finish_bwd(pre, gain, cos_t, sin_t, d_rot):
    d_normed = d_rot * cos_t - half_roll(d_rot) * sin_t
    scale = row_scale(pre)
    unit = pre * scale
    d_unit = d_normed * gain
    return scale * (d_unit - unit * row_mean(d_unit * unit)), d_normed * unit


def slot_of(tok):
    return ((tok // 4) * 2 + tok % 2) * 2 + (tok // 2) % 2


PATHS = "t2m4m8m124282184684181" + "61a1c1e1"
HOPS = tuple(zip(PATHS[::2], (int(flip) for flip in PATHS[1::2])))


def place_of(source):
    return 0 if source in "tm" else int(source, 16)


def gather_kernel(steps, x_ref, gain_ref, wq_ref, wk_ref, wv_ref, freq_ref, local_ref, other_ref, qpre_ref, kpre_ref, cos_ref, sin_ref, w_ref, all_ref, swap_ref, h_ref, send, recv, own, swap_send, swap_recv):
    step = grid_step()
    me = lax.axis_index('cp')
    which = (me // 2) % 2
    mesh_id = pl.DeviceIdType.MESH

    def hop(n):
        source, flip = HOPS[n]
        block = me ^ place_of(source)
        src = local_ref.at[which] if source == "m" else local_ref.at[1 - which] if source == "t" else all_ref.at[block]
        return pltpu.make_async_remote_copy(src_ref=src, dst_ref=all_ref.at[block], send_sem=send.at[n], recv_sem=recv.at[n], device_id=(me ^ flip,), device_id_type=mesh_id)

    mine = pltpu.make_async_copy(local_ref.at[which], all_ref.at[me], own)
    swap = pltpu.make_async_remote_copy(src_ref=other_ref.at[1 - which], dst_ref=swap_ref, send_sem=swap_send, recv_sem=swap_recv, device_id=(me ^ 2,), device_id_type=mesh_id)

    @pl.when(step == 0)
    def _():
        meet(me, sorted({flip for _, flip in HOPS}))
        for n, (source, _) in enumerate(HOPS):
            if source in "tm":
                hop(n).start()
        mine.start()
        rows = x_ref.shape[1]
        for b in range(2):
            for first in range(0, rows, 128):
                x = x_ref[b, first:first + 128].astype(F32)
                scale = row_scale(x)
                h_ref[b * rows + first:b * rows + first + 128] = (x * scale * gain_ref[:]).astype(BF16)

    @pl.when(step < steps - 1)
    def _():
        qpre_ref[:] = nn(h_ref[:], wq_ref[:])
        span = cos_ref.shape[0]
        position = (step * span + lax.broadcasted_iota(jnp.int32, (span, HEAD_DIM), 0)).astype(F32)
        angles = position * freq_ref[:]
        cos_ref[:] = jnp.cos(angles)
        lower = lax.broadcasted_iota(jnp.int32, (span, HEAD_DIM), 1) < HEAD_DIM // 2
        sine = jnp.sin(angles)
        sin_ref[:] = jnp.where(lower, -sine, sine)

    group, half = me // 4, me % 2
    for j in range(2):
        for core in range(2):
            @pl.when((step == 2 * group + j) & (half == core))
            def _():
                for c in range(2):
                    w_ref[:, lanes(2 * c + j)] = wq_ref[:, lanes(2 * core + c)]
    for n in range(4):
        @pl.when((step == 0) & (group == n))
        def _():
            w_ref[:, lanes(4)] = wk_ref[:, lanes(n)]
            w_ref[:, lanes(5)] = wv_ref[:, lanes(n)]

    @pl.when(step == steps - 1)
    def _():
        kpre_ref[:] = nn(h_ref[:], wk_ref[:])
        for n, (source, flip) in enumerate(HOPS):
            if flip > 1:
                hop(n).wait_recv()
                for then, (needs, _) in enumerate(HOPS):
                    if needs not in "tm" and place_of(needs) == place_of(source) ^ flip:
                        hop(then).start()
                if source == "t":
                    swap.start()
        for n, (_, flip) in enumerate(HOPS):
            if flip == 1:
                hop(n).wait_recv()
        for n in range(len(HOPS)):
            hop(n).wait_send()
        mine.wait()
        swap.wait()


def run_gather(hidden_in, grad_out, gain, w_query, w_key, w_value, freq, seq, key):
    batch, rows, dim = hidden_in.shape
    width = w_key.shape[1]
    steps = w_query.shape[1] // width + 1
    tile = lambda t: (0, jnp.minimum(t, steps - 2))
    hbm = pl.BlockSpec(memory_space=pltpu.HBM)
    sds = jax.ShapeDtypeStruct
    one, count = pltpu.SemaphoreType.DMA, pltpu.SemaphoreType.DMA((len(HOPS),))
    both = batch * rows
    table = pl.BlockSpec((seq // (steps - 1), HEAD_DIM), lambda t: (jnp.minimum(t, steps - 2), 0))
    return pl.pallas_call(
        functools.partial(gather_kernel, steps), grid=(steps,), name="gather",
        in_specs=[whole(hidden_in), whole(gain), pl.BlockSpec((dim, width), tile), whole(w_key), whole(w_value), whole(freq), hbm, hbm],
        out_specs=[pl.BlockSpec((both, width), tile), fixed(both, width), table, table, fixed(dim, 6 * HEAD_DIM), hbm, hbm],
        out_shape=[sds((both, w_query.shape[1]), F32), sds((both, width), F32), sds((seq, HEAD_DIM), F32), sds((seq, HEAD_DIM), F32), sds((dim, 6 * HEAD_DIM), BF16), sds((16, rows, dim), BF16), sds((rows, dim), BF16)],
        scratch_shapes=[pltpu.VMEM((both, dim), BF16), count, count, one, one, one],
        compiler_params=params(collective_id=key, has_side_effects=True), cost_estimate=cost(2 * both * dim * 4608, 60000000),
    )(hidden_in, gain, w_query, w_key, w_value, freq, hidden_in, grad_out)


def qkv_kernel(x_ref, gain_ref, w_ref, qn_ref, kn_ref, cos_ref, sin_ref, h_ref, qpre_ref, kpre_ref, q_ref, k_ref, kt_ref, v_ref, vt_ref):
    for first in range(0, x_ref.shape[0], 128):
        rs = slice(first, first + 128)
        x = x_ref[rs].astype(F32)
        scale = row_scale(x)
        h = (x * scale * gain_ref[:]).astype(BF16)
        h_ref[rs] = h
        pre = nn(h, w_ref[:])
        cos_t, sin_t = cos_ref[rs], sin_ref[rs]
        qpre_ref[rs] = pre[:, :4 * HEAD_DIM]
        for head in range(4):
            q_ref[rs, lanes(head)] = head_finish(pre[:, lanes(head)], qn_ref[:], cos_t, sin_t).astype(BF16)
        kpre = pre[:, lanes(4)]
        kpre_ref[rs] = kpre
        k_rot = head_finish(kpre, kn_ref[:], cos_t, sin_t)
        k_ref[rs] = k_rot.astype(BF16)
        kt_ref[:, rs] = k_rot.T.astype(BF16)
        v = pre[:, lanes(5)]
        v_ref[rs] = v.astype(BF16)
        vt_ref[:, rs] = v.T.astype(BF16)


def run_qkv(x, gain, w_all, qn, kn, cos_t, sin_t):
    seq, dim = x.shape
    rows = 512
    row = lambda width: row_spec(rows, width)
    col = pl.BlockSpec((HEAD_DIM, rows), lambda t: (0, t))
    sds = jax.ShapeDtypeStruct
    return pl.pallas_call(
        qkv_kernel, grid=(seq // rows,), name="qkv",
        in_specs=[row(dim), whole(gain), whole(w_all), whole(qn), whole(kn), row(HEAD_DIM), row(HEAD_DIM)],
        out_specs=[row(dim), row(4 * HEAD_DIM), row(HEAD_DIM), row(4 * HEAD_DIM), row(HEAD_DIM), col, row(HEAD_DIM), col],
        out_shape=[sds((seq, dim), BF16), sds((seq, 4 * HEAD_DIM), F32), sds((seq, HEAD_DIM), F32), sds((seq, 4 * HEAD_DIM), BF16),
                   sds((seq, HEAD_DIM), BF16), sds((HEAD_DIM, seq), BF16), sds((seq, HEAD_DIM), BF16), sds((HEAD_DIM, seq), BF16)],
        compiler_params=params(), cost_estimate=cost(2 * seq * dim * 768, seq * dim * 8),
    )(x, gain, w_all, qn, kn, cos_t, sin_t)


def out_grad_kernel(g_ref, w_ref, o_ref, do_ref, wg_ref):
    @pl.when(grid_step() == 0)
    def _():
        wg_ref[:] = jnp.zeros_like(wg_ref)

    g = g_ref[0]
    do_ref[:] = nn(g, w_ref[:]).astype(BF16)
    wg_ref[:] += tn(o_ref[:], g)


def run_out_grad(gg, wo, o):
    blocks, rows, dim = gg.shape
    width = wo.shape[1]
    row = row_spec(rows, width)
    return pl.pallas_call(
        out_grad_kernel, grid=(blocks,), name="out_grad",
        in_specs=[pl.BlockSpec((1, rows, dim), lambda t: (slot_of(t), 0, 0)), whole(wo), row], out_specs=[row, fixed(width, dim)],
        out_shape=[jax.ShapeDtypeStruct(o.shape, BF16), jax.ShapeDtypeStruct((width, dim), F32)],
        compiler_params=params(), cost_estimate=cost(4 * blocks * rows * dim * width, blocks * rows * dim * 2),
    )(gg, wo, o)


def q_grad_kernel(dq_ref, qpre_ref, qn_ref, cos_ref, sin_ref, h_ref, wg_ref, dt_ref):
    @pl.when(grid_step() == 0)
    def _():
        wg_ref[:] = jnp.zeros_like(wg_ref)
        dt_ref[:] = jnp.zeros_like(dt_ref)

    wg_ref[:] += nn(dt_ref[:], h_ref[:])
    cos_t, sin_t = cos_ref[:], sin_ref[:]
    for head in range(2):
        d_pre, _ = head_finish_bwd(qpre_ref[:, lanes(head)], qn_ref[:], cos_t, sin_t, dq_ref[:, lanes(head)].astype(F32))
        dt_ref[lanes(head), :] = d_pre.T.astype(BF16)


def run_q_grad(dq, qpre, chunk, qn, cos_t, sin_t, h, carry=(), key=None):
    seq, dim = h.shape
    rows, height = 512, 256
    count = seq // rows
    row = lambda width, c=0: pl.BlockSpec((rows, width), lambda t: (jnp.minimum(t, count - 1), c))
    specs = [row(256), row(256, chunk), whole(qn), row(HEAD_DIM), row(HEAD_DIM), pl.BlockSpec((rows, dim), lambda t: (jnp.maximum(t - 1, 0), 0))]
    return call(q_grad_kernel, count + 1, specs, [fixed(height, dim)], [jax.ShapeDtypeStruct((height, dim), F32)],
                [pltpu.VMEM((height, rows), BF16)], cost(2 * seq * dim * height, seq * dim * 3), (dq, qpre, qn, cos_t, sin_t, h), carry, key)


def kv_grad_kernel(count, dk_ref, dv_ref, got_ref, kpre_ref, kn_ref, cos_ref, sin_ref, h_ref, o0_ref, o1_ref, wo_ref, kvb_ref, sum_ref, out_ref, dt_ref, acc_ref, land_ref, send, recv):
    step = grid_step()
    me = lax.axis_index('cp')
    is_key = me % 2 == 0
    rows = land_ref.shape[0]
    theirs = pl.multiple_of((1 - (me // 2) % 2) * rows, rows)
    ours = pl.multiple_of((me // 2) % 2 * rows, rows)

    @pl.when(step == 0)
    def _():
        acc_ref[:] = jnp.zeros_like(acc_ref)
        dt_ref[:] = jnp.zeros_like(dt_ref)
        out_ref[:] = jnp.zeros_like(out_ref)

    @pl.when(step <= count)
    def _():
        acc_ref[:] += nn(dt_ref[:], h_ref[:])
        kv = (jnp.where(is_key, dk_ref[:], dv_ref[:]) + got_ref[:]).T.astype(BF16)
        kvb_ref[:] = kv
        dk_pre, _ = head_finish_bwd(kpre_ref[:], kn_ref[:], cos_ref[:], sin_ref[:], kv.astype(F32))
        dt_ref[:] = jnp.where(step < count, jnp.where(is_key, dk_pre, kv.astype(F32)).T, jnp.zeros_like(dk_pre.T)).astype(BF16)

    tokens = o0_ref.shape[3]
    for j in range(2):
        @pl.when(step % 2 == j)
        def _():
            for b in range(2):
                pair = jnp.hstack([o0_ref[0, b, 0][:, lanes(j)], o1_ref[0, b, 0][:, lanes(j)]])
                out_ref[b * tokens:(b + 1) * tokens] += nn(pair, wo_ref[:])

    copy = pltpu.make_async_remote_copy(src_ref=acc_ref.at[pl.ds(theirs, rows)], dst_ref=land_ref, send_sem=send, recv_sem=recv,
                                        device_id=(me ^ 2,), device_id_type=pl.DeviceIdType.MESH)

    @pl.when(step == count + 1)
    def _():
        copy.start()

    @pl.when(step == pl.num_programs(0) - 1)
    def _():
        copy.wait()
        sum_ref[:] = acc_ref[pl.ds(ours, rows), :] + land_ref[:]


def run_kv_grad(dk, dv, got, kpre, kn, cos_t, sin_t, h, o_got, w_out, carry, key):
    seq, dim = h.shape
    rows = 512
    count = seq // rows
    tokens = o_got[0].shape[3]
    last = lambda t: jnp.minimum(t, count - 1)
    col = pl.BlockSpec((HEAD_DIM, rows), lambda t: (0, last(t)))
    row = pl.BlockSpec((rows, HEAD_DIM), lambda t: (last(t), 0))
    src = pl.BlockSpec((1, 2, 1, tokens, 256), lambda s: (s // 4, 0, (s // 2) % 2, 0, 0))
    specs = [col, col, col, row, whole(kn), row, row, pl.BlockSpec((rows, dim), lambda t: (jnp.clip(t - 1, 0, count - 1), 0)),
             src, src, pl.BlockSpec((256, dim), lambda s: (4 * (s // 4) + 2 * (s % 2) + (s // 2) % 2, 0))]
    sds = jax.ShapeDtypeStruct
    half, both = HEAD_DIM // 2, 2 * tokens
    return call(functools.partial(kv_grad_kernel, count), 16, specs, [row, fixed(half, dim), fixed(both, dim)],
                [sds((seq, HEAD_DIM), BF16), sds((half, dim), F32), sds((both, dim), F32)],
                [pltpu.VMEM((HEAD_DIM, rows), BF16), pltpu.VMEM((HEAD_DIM, dim), F32), pltpu.VMEM((half, dim), F32), pltpu.SemaphoreType.DMA, pltpu.SemaphoreType.DMA],
                cost(2 * seq * dim * 768, seq * dim * 2), (dk, dv, got, kpre, kn, cos_t, sin_t, h, *o_got, w_out), carry, key)


def hidden_grad_kernel(final, dq_ref, qa_ref, qb_ref, wa_ref, wb_ref, qn_ref, cos_ref, sin_ref, *refs):
    if final:
        kv_ref, kpre_ref, wk_ref, wv_ref, kn_ref, gain_ref, x_ref, g_ref, so_far_ref, dx_ref, ngq_ref, ngk_ref, ngx_ref, acc_ref, d_ref, w_ref = refs
    else:
        acc_ref, ngq_ref, d_ref = refs
    step = grid_step()
    rows = dq_ref.shape[3]

    @pl.when(step == 0)
    def _():
        acc_ref[:] = so_far_ref[:] if final else jnp.zeros_like(acc_ref)
        ngq_ref[:] = jnp.zeros_like(ngq_ref)
        if final:
            ngk_ref[:] = jnp.zeros_like(ngk_ref)
            ngx_ref[:] = jnp.zeros_like(ngx_ref)

    is_key = step % 2 == 0
    if final:
        w_ref[:] = jnp.where(is_key, wk_ref[:].astype(F32), wv_ref[:].astype(F32)).astype(BF16)
    folded = lambda terms: jnp.sum(terms.reshape(-1, 8, terms.shape[1]), axis=0)
    for b in range(2):
        for first in range(0, rows, HEAD_DIM):
            rs, at = slice(first, first + HEAD_DIM), slice(b * rows + first, b * rows + first + HEAD_DIM)
            cos_t, sin_t = cos_ref[rs], sin_ref[rs]
            for j, q_ref in enumerate((qa_ref, qb_ref)):
                d_pre, terms = head_finish_bwd(q_ref[at], qn_ref[:], cos_t, sin_t, dq_ref[0, b, 0, rs, lanes(j)].astype(F32))
                d_ref[at, lanes(j)] = d_pre.astype(BF16)
                ngq_ref[:] += folded(terms)
            if final:
                kv = kv_ref[0, b, 0, rs].astype(F32)
                dk_pre, terms = head_finish_bwd(kpre_ref[at], kn_ref[:], cos_t, sin_t, kv)
                ngk_ref[:] += jnp.where(is_key, folded(terms), jnp.zeros_like(ngk_ref))
                d_ref[at, lanes(2)] = jnp.where(is_key, dk_pre, kv).astype(BF16)
        at = slice(b * rows, (b + 1) * rows)
        for first in range(0, acc_ref.shape[1], 512):
            cols = slice(first, first + 512)
            part = nt(d_ref[at, :2 * HEAD_DIM], jnp.hstack([wa_ref[cols], wb_ref[cols]]))
            acc_ref[at, cols] += part + nt(d_ref[at, lanes(2)], w_ref[cols]) if final else part
    if not final:
        return

    @pl.when(step == pl.num_programs(0) - 1)
    def _():
        for b in range(2):
            for r in range(0, rows, 64):
                rs = slice(r, r + 64)
                x = x_ref[b, rs].astype(F32)
                scale = row_scale(x)
                unit = x * scale
                d_normed = acc_ref[b * rows + r:b * rows + r + 64, :].astype(BF16).astype(F32)
                ngx_ref[:] += folded(d_normed * unit)
                d_unit = d_normed * gain_ref[:]
                dx_ref[b, rs] = (g_ref[b, rs].astype(F32) + scale * (d_unit - unit * row_mean(d_unit * unit))).astype(BF16)


def run_hidden_grad(dq_got, chunk, qpre_own, w_query, qn, cos_t, sin_t, rest=None, carry=(), key=None):
    rows, dim = dq_got.shape[3], w_query.shape[0]
    both = 2 * rows
    src = lambda width: pl.BlockSpec((1, 2, 1, rows, width), lambda s: (s // 2, 0, s % 2, 0, 0))
    head = lambda height, j: pl.BlockSpec((height, HEAD_DIM), lambda s: (0, 8 * (s // 2) + 4 * j + 2 * (s % 2) + chunk))
    group = lambda height: pl.BlockSpec((height, HEAD_DIM), lambda s: (0, s // 2))
    sds = jax.ShapeDtypeStruct
    norm = sds((8, HEAD_DIM), F32)
    specs = [src(2 * HEAD_DIM), head(both, 0), head(both, 1), head(dim, 0), head(dim, 1), whole(qn), whole(cos_t), whole(sin_t)]
    operands = (dq_got, qpre_own, qpre_own, w_query, w_query, qn, cos_t, sin_t)
    outs = [sds((both, dim), F32), norm]
    scratch = [pltpu.VMEM((both, 3 * HEAD_DIM), BF16)]
    if rest is not None:
        _, _, _, _, kn, gain, hidden_in, grad_out, so_far = rest
        operands += rest
        specs += [src(HEAD_DIM), group(both), group(dim), group(dim), whole(kn), whole(gain), whole(hidden_in), whole(grad_out), whole(so_far)]
        outs = [sds(hidden_in.shape, BF16), norm, norm, sds((8, dim), F32)]
        scratch = [pltpu.VMEM((both, dim), F32)] + scratch + [pltpu.VMEM((dim, HEAD_DIM), BF16)]
    return call(functools.partial(hidden_grad_kernel, rest is not None), 8, specs, [fixed(*out.shape) for out in outs], outs, scratch,
                cost(2 * both * dim * 2560, 30000000), operands, carry, key)


def place_kernel(*refs):
    refs[-1][:] = refs[0][0].T


def run_place(a, chunk, into=None):
    count, height, dim = a.shape[0], HEAD_DIM, a.shape[2]
    more = [] if into is None else [into]
    return pl.pallas_call(
        place_kernel, grid=(count,), name="place",
        in_specs=[pl.BlockSpec((1, height, dim), lambda t: (t, 0, 0))] + [pl.BlockSpec(memory_space=pltpu.HBM)] * len(more),
        out_specs=pl.BlockSpec((dim, height), lambda t: (0, 2 * t + chunk)), input_output_aliases={} if into is None else {1: 0},
        out_shape=jax.ShapeDtypeStruct((dim, 2 * height * count), F32), compiler_params=params(), cost_estimate=cost(1000000, 35000000),
    )(a, *more)


def join_kernel(a_ref, b_ref, y_ref):
    for n in range(a_ref.shape[0]):
        y_ref[2 * n * HEAD_DIM:(2 * n + 1) * HEAD_DIM] = a_ref[n]
        y_ref[(2 * n + 1) * HEAD_DIM:(2 * n + 2) * HEAD_DIM] = b_ref[n]


def run_join(a, b):
    count, height, dim = a.shape
    spec = pl.BlockSpec((2, height, dim), lambda t: (t, 0, 0))
    return pl.pallas_call(
        join_kernel, grid=(count // 2,), name="join", in_specs=[spec, spec], out_specs=pl.BlockSpec((4 * height, dim), lambda t: (t, 0)),
        out_shape=jax.ShapeDtypeStruct((2 * height * count, dim), F32), compiler_params=params(), cost_estimate=cost(1000000, 67000000),
    )(a, b)


def place_kv_kernel(*refs):
    half = HEAD_DIM // 2
    for out in range(2):
        for b in range(2):
            refs[4 + out][:, b * half:(b + 1) * half] = refs[2 * out + b][0].T


def run_place_kv(a):
    dim = a.shape[2]
    source = lambda out, b: pl.BlockSpec((1, HEAD_DIM // 2, dim), lambda g: (4 * g + 2 * b + out, 2, 0))
    spec = pl.BlockSpec((dim, HEAD_DIM), lambda g: (0, g))
    shape = jax.ShapeDtypeStruct((dim, 4 * HEAD_DIM), F32)
    return pl.pallas_call(
        place_kv_kernel, grid=(4,), name="place_kv", in_specs=[source(out, b) for out in range(2) for b in range(2)], out_specs=[spec, spec],
        out_shape=[shape, shape], compiler_params=params(), cost_estimate=cost(1000000, 17000000),
    )(a, a, a, a)


def sum_kernel(x_ref, y_ref, land_ref, send, recv, own):
    me = lax.axis_index('cp')
    meet(me, FLIPS["all"])
    copies = [pltpu.make_async_remote_copy(src_ref=x_ref, dst_ref=land_ref.at[me], send_sem=send.at[n], recv_sem=recv.at[n], device_id=(me ^ flip,),
                                           device_id_type=pl.DeviceIdType.MESH) for n, flip in enumerate(FLIPS["all"])]
    copies.append(pltpu.make_async_copy(x_ref, land_ref.at[me], own))
    for copy in copies:
        copy.start()
    for copy in copies:
        copy.wait()
    total = land_ref[0]
    for n in range(1, 16):
        total = total + land_ref[n]
    y_ref[:] = total


def run_sum(x, key):
    count = pltpu.SemaphoreType.DMA((15,))
    return pl.pallas_call(
        sum_kernel, name="sum", in_specs=[pl.BlockSpec(memory_space=pltpu.HBM)], out_specs=pl.BlockSpec(memory_space=pltpu.VMEM),
        out_shape=jax.ShapeDtypeStruct(x.shape, F32), scratch_shapes=[pltpu.VMEM((16,) + x.shape, F32), count, count, pltpu.SemaphoreType.DMA],
        compiler_params=pltpu.CompilerParams(collective_id=key, has_side_effects=True), cost_estimate=cost(1000000, 1000000),
    )(x)


def solution(mesh):
    n_dev = mesh.shape['cp']
    seq_spec, rep_spec = P(None, 'cp', None), P()
    halves = [[dev for dev in range(n_dev) if (dev >> 1) & 1 == bit] for bit in (0, 1)]

    def local_block(hidden_in, grad_out, w_query, w_key, w_value, w_out, attn_norm, query_norm, key_norm):
        _, seq_dev, dim = hidden_in.shape
        seq = seq_dev * n_dev
        me = lax.axis_index('cp')
        group, which, half = me // 4, (me // 2) % 2, me % 2
        gain = attn_norm.astype(F32).reshape(1, dim)
        qn, kn = query_norm.astype(F32).reshape(1, HEAD_DIM), key_norm.astype(F32).reshape(1, HEAD_DIM)
        keys = iter(range(1, 16))
        blocks = lambda x: x.reshape(-1, seq_dev, x.shape[1])
        by_source = lambda x: x.reshape(4, 2, 2, seq_dev, x.shape[2])
        gather_all = lambda x: lax.all_gather(x, 'cp')
        add_half = lambda parts, got: lax.dynamic_slice_in_dim(parts, which * HEAD_DIM, HEAD_DIM) + got

        qpre_own, kpre_own, cos_t, sin_t, w_all, xg, g_got = run_gather(hidden_in, grad_out, gain, w_query, w_key, w_value, inverse_frequencies(), seq, next(keys))

        head_at = lambda c, j: (8 * group + 4 * j + 2 * half + c) * HEAD_DIM
        wo_mine = [jnp.concatenate([lax.dynamic_slice_in_dim(w_out, head_at(c, j), HEAD_DIM) for j in range(2)]).T for c in range(2)]

        pair = lax.dynamic_update_index_in_dim(grad_out, g_got, 1 - which, 0)
        gg = lax.all_gather(pair, 'cp', axis_index_groups=halves, tiled=True)

        h, qpre, kpre, q, k, kt, v, vt = run_qkv(xg.reshape(seq, dim), gain, w_all, qn, kn, cos_t, sin_t)
        o0, lse0 = run_fwd(q, kt, v, 0)
        do0, wg_o0 = run_out_grad(gg, wo_mine[0], o0)
        dq0, dkt0, dvt0, got = run_bwd(q, do0, o0, lse0, kt, vt, k, 0, [("half", wg_o0)], next(keys), (), (0, 6), False, 'new')
        mine, dkt0 = lax.optimization_barrier((add_half(wg_o0, got), dkt0))
        wg_o0 = gather_all(mine)
        dq0, dkt0, dvt0, o_got0 = run_bwd(q, do0, o0, lse0, kt, vt, k, 0, [("all", blocks(o0))], next(keys), (dkt0, dvt0), (6, 12), False, dq0)
        wg_q0, = run_q_grad(dq0, qpre, 0, qn, cos_t, sin_t, h)

        q, wg_q0 = lax.optimization_barrier((q, wg_q0))
        o1, lse1, got, dq_got0 = run_fwd(q, kt, v, 1, [("half", wg_q0), ("all", blocks(dq0))], next(keys), (0, 9))
        mine, o1 = lax.optimization_barrier((add_half(wg_q0, got), o1))
        wg_q0 = gather_all(mine)
        o1, lse1 = run_fwd(q, kt, v, 1, (), None, (9, 12), (o1, lse1))
        do1, wg_o1 = run_out_grad(gg, wo_mine[1], o1)
        dq1a, dkt, dvt, got, o_got1 = run_bwd(q, do1, o1, lse1, kt, vt, k, 1, [("half", wg_o1), ("all", blocks(o1))], next(keys), (dkt0, dvt0), (0, 9))
        mine, dkt = lax.optimization_barrier((add_half(wg_o1, got), dkt))
        wg_o1 = gather_all(mine)
        dq1b, dkt, dvt, low = run_bwd(q, do1, o1, lse1, kt, vt, k, 1, [("low", blocks(dq1a))], next(keys), (dkt, dvt), (9, 12), True)

        wg_q1, kv_part = run_q_grad(jnp.concatenate([dq1a, dq1b]), qpre, 1, qn, cos_t, sin_t, h, [("other", dkt, dvt)], next(keys))
        kv_b, kv_sum, projected, got = run_kv_grad(dkt, dvt, kv_part, kpre, kn, cos_t, sin_t, h, [by_source(o_got0), by_source(o_got1)], w_out, [("half", wg_q1)], next(keys))
        mine, kv_b = lax.optimization_barrier((jnp.concatenate([add_half(wg_q1, got), kv_sum]), kv_b))
        wg_q1 = gather_all(mine)
        my_cos, my_sin = [lax.dynamic_slice_in_dim(table, me * seq_dev, seq_dev) for table in (cos_t, sin_t)]
        so_far, ng_q0, high, kv_got = run_hidden_grad(by_source(dq_got0), 0, qpre_own, w_query, qn, my_cos, my_sin, None, [("high", blocks(dq1b)), ("all", blocks(kv_b))], next(keys))
        dq_got1 = by_source(jnp.where(me < SPLIT, low, high))
        rest = (by_source(kv_got), kpre_own, w_key, w_value, kn, gain, hidden_in, grad_out, so_far)
        grad_in, ng_q1, ng_k, ng_x = run_hidden_grad(dq_got1, 1, qpre_own, w_query, qn, my_cos, my_sin, rest)
        hidden_out = (hidden_in.astype(F32) + projected.reshape(hidden_in.shape)).astype(BF16)
        wgrad_out = run_join(wg_o0, wg_o1)
        wgrad_q = run_place(wg_q1, 1, run_place(wg_q0, 0))
        wgrad_k, wgrad_v = run_place_kv(wg_q1)
        norms = jnp.sum(jnp.hstack([ng_x, ng_q0 + ng_q1, ng_k]), axis=0, keepdims=True)
        norms, wgrad_k = lax.optimization_barrier((norms, wgrad_k))
        norms = run_sum(norms, next(keys))[0]
        return (hidden_out, grad_in, wgrad_q, wgrad_k, wgrad_v, wgrad_out,
                norms[:dim], norms[dim:dim + HEAD_DIM], norms[dim + HEAD_DIM:])

    return jax.shard_map(local_block, mesh=mesh, in_specs=(seq_spec, seq_spec) + (rep_spec,) * 7, out_specs=(seq_spec, seq_spec) + (rep_spec,) * 7, check_vma=False)
```
